32 devices in a mesh: gx: 4 (over z), gy: 4 (over x, core), gz: 2 (over y).
Axes of the slice: x: 2, y: 2, z: 4, core: 2. Of those that a mesh axis runs over, the one named last changes fastest.
Arguments:
- models: float32 [2, 64, 128, 256], P(None, 'gx', 'gy', 'gz'), may hold values from -6 to 6
- targets: float32 [2, 64, 128, 256], P(None, 'gx', 'gy', 'gz'), may hold values from -6 to 6
- weights: float32 [2, 64, 128, 256], P(None, 'gx', 'gy', 'gz'), may hold values from 0.5 to 12, as said below
Outputs:
- updated: float32 [2, 64, 128, 256], P(None, 'gx', 'gy', 'gz')
- applied_last: float32 [2, 64, 128, 256], P(None, 'gx', 'gy', 'gz')
The draws below stay inside these ranges and needn't reach their ends.
Inputs may be any that keep to these rules, and one draw needn't show every extreme that they name: Positive data weights.
All inputs are finite; a program needn't handle non-finite values.
Results may differ from the reference program's by a relative error of at most 0.00016.
Values sent between devices are 32-bit elements; how exact they have to be, the bound alone decides.
A program may use at most 128 MiB of HBM per device.

```python
import math
import jax
import jax.numpy as jnp
from jax import lax

ITERS = 3
NX = 64
NY = 128
NZ = 256


def draw_weights(key, part):
    base_key = jax.random.fold_in(key, 11)
    base = jnp.exp(jax.random.uniform(base_key, (2, NX, NY, NZ), jnp.float32, math.log(0.5), math.log(4.0)))
    ramp = 1.0 + 2.0 * jnp.arange(NX, dtype=jnp.float32) / max(NX - 1, 1)
    return base * ramp[None, :, None, None]


def levels(stream_key, extent, shards, least, high):
    loudness, own = 1.0, jax.random.fold_in(stream_key, 6)
    for dim, parts in shards:
        heights = jnp.exp(jax.random.uniform(jax.random.fold_in(own, dim), (parts,), jnp.float32, least / len(shards), high / len(shards)))
        loudness = loudness * jnp.repeat(heights, extent[dim] // parts).reshape([-1 if axis == dim else 1 for axis in range(len(extent))])
    return loudness


def normal_values(key, shape, width, reach, shards=(), held_as=jnp.bfloat16):
    drawn = jax.random.normal(key, shape, jnp.float32) * width
    if len(shards) > 0:
        drawn = levels(key, shape, shards, -0.22, 0.18) * drawn
    return jnp.clip(drawn, min=-reach, max=reach).astype(held_as)


def setup_inputs(seed: int = 0) -> dict:
    splits = jax.random.split(jax.random.key(seed), 4)
    models = normal_values(splits[0], (2, NX, NY, NZ), 1.0, 6.0, ((1, 4), (2, 4), (3, 2)), jnp.float32)
    targets = normal_values(splits[1], (2, NX, NY, NZ), 1.0, 6.0, ((1, 4), (2, 4), (3, 2)), jnp.float32)
    weights = draw_weights(jax.random.fold_in(splits[3], 71), 0)
    return dict(models=models, targets=targets, weights=weights)


def central(field, which):
    length = field.shape[which]
    widths = [(1, 1) if k == which else (0, 0) for k in range(3)]
    padded = jnp.pad(field, widths)
    upper = lax.slice_in_dim(padded, 2, length + 2, axis=which)
    lower = lax.slice_in_dim(padded, 0, length, axis=which)
    return 0.5 * (upper - lower)


def laplace(field):
    summed = 6.0 * field
    for which in range(3):
        length = field.shape[which]
        widths = [(1, 1) if k == which else (0, 0) for k in range(3)]
        padded = jnp.pad(field, widths)
        summed = summed - lax.slice_in_dim(padded, 2, length + 2, axis=which) - lax.slice_in_dim(padded, 0, length, axis=which)
    return summed


def vector_cross(first_vec, second_vec):
    return (first_vec[1] * second_vec[2] - first_vec[2] * second_vec[1],
            first_vec[2] * second_vec[0] - first_vec[0] * second_vec[2],
            first_vec[0] * second_vec[1] - first_vec[1] * second_vec[0])


def reference(models, targets, weights):
    current = models
    applied = jnp.zeros_like(models)
    for iteration in range(ITERS):
        first_grad = [central(current[0], k) for k in range(3)]
        second_grad = [central(current[1], k) for k in range(3)]
        crossed = vector_cross(first_grad, second_grad)
        first_flux = vector_cross(second_grad, crossed)
        second_flux = vector_cross(crossed, first_grad)
        first_coupling = -2.0 * (central(first_flux[0], 0) + central(first_flux[1], 1) + central(first_flux[2], 2))
        second_coupling = -2.0 * (central(second_flux[0], 0) + central(second_flux[1], 1) + central(second_flux[2], 2))
        smooth = jnp.stack([laplace(current[0]), laplace(current[1])])
        coupling = jnp.stack([first_coupling, second_coupling])
        gradient = weights * (current - targets) + 1.0 * smooth + 0.05 * coupling
        grad_norm = jnp.sum(gradient * gradient)
        applied = weights * gradient + 1.0 * jnp.stack([laplace(gradient[0]), laplace(gradient[1])])
        curvature = jnp.sum(gradient * applied)
        current = current - (grad_norm / curvature) * gradient
    return (current, applied)
```

```python
import functools

import jax
import jax.numpy as jnp
from jax import lax
from jax.experimental import pallas as pl
from jax.experimental.pallas import tpu as pltpu
from jax.sharding import PartitionSpec as P

ITERS = 3
AXES = ("gx", "gy", "gz")
MESH = pl.DeviceIdType.MESH
X1, X2, Y, Z, YE, ZE = 0, 2, 4, 6, 8, 10
COUPLE = -2.0 * 0.05 / 16.0


def kernel(sizes, models, targets, weights, updated, applied, cur, grad, zcur, zgrad, pack, f0, f1, f2, fz,
           ysend, yrecv, yesend, yerecv, zsend, zrecv, red, send, recv, red_send, red_recv):
    nx, ny, nz = sizes
    total = nx * ny * nz
    _, cells_x, cells_y, lanes = models.shape
    low, high = 8, 8 + cells_y
    own = pl.ds(low, cells_y)
    ix, iy, iz = (lax.axis_index(axis) for axis in AXES)
    here = (ix, iy, iz)
    me = (ix * ny + iy) * nz + iz
    lane_row = lax.broadcasted_iota(jnp.int32, (1, lanes), 1)
    slot = lax.rem(lane_row, 4)

    def has(axis, direction):
        return here[axis] > 0 if direction == 0 else here[axis] < sizes[axis] - 1

    def copy(step, axis, direction, kind, src, dst):
        there = list(here)
        there[axis] = here[axis] + (1 if direction else -1)
        return pltpu.make_async_remote_copy(
            src_ref=src, dst_ref=dst, send_sem=send.at[step, kind + direction], recv_sem=recv.at[step, kind + direction],
            device_id=tuple(there), device_id_type=MESH)

    def transfers(step, field):
        made = {}
        for direction in range(2):
            near, far = (2, cells_x + 2) if direction == 0 else (cells_x + 1, 1)
            made[X1, direction] = (0, field.at[:, near, own], field.at[:, far, own])
            near, far = (3, cells_x + 3) if direction == 0 else (cells_x, 0)
            made[X2, direction] = (0, field.at[:, near, own], field.at[:, far, own])
            made[Y, direction] = (1, ysend.at[step, direction], yrecv.at[step, direction])
            made[YE, direction] = (1, yesend.at[step, direction], yerecv.at[step, direction])
            made[Z, direction] = (2, zsend.at[step, 0], zrecv.at[step, 0, direction])
            made[ZE, direction] = (2, zsend.at[step, 1], zrecv.at[step, 1, direction])
        return {key: (value[0], copy(step, value[0], key[1], key[0], value[1], value[2])) for key, value in made.items()}

    def start(made, kind):
        for direction in range(2):
            axis, move = made[kind, direction]

            @pl.when(has(axis, direction))
            def _():
                move.start()

    def arrive(made, kind):
        for direction in range(2):
            axis, move = made[kind, direction]

            @pl.when(has(axis, 1 - direction))
            def _():
                move.wait_recv()

    def sent(made, kind):
        for direction in range(2):
            axis, move = made[kind, direction]

            @pl.when(has(axis, direction))
            def _():
                move.wait_send()

    def pack_z(field, step, which):
        group = lane_row // 4

        def body(xi, carry):
            return tuple(
                jnp.where(group == xi, pltpu.roll(field[m, xi], 4 * xi + 2, 1), carry[m]) for m in range(2))

        zero = jnp.zeros(field.shape[2:], jnp.float32)
        edge = 2 if which == 0 else 1
        packed = lax.fori_loop(edge, cells_x + 4 - edge, body, (zero, zero))
        for m in range(2):
            v = packed[m]
            pack[m] = v
            turned = jnp.where(slot == 0, pltpu.roll(v, lanes - 3, 1), pltpu.roll(v, 3, 1))
            turned = jnp.where(slot == 1, pltpu.roll(v, lanes - 1, 1), turned)
            zsend[step, which, m] = jnp.where(slot == 2, pltpu.roll(v, 1, 1), turned)

    def unpack_z(zfield, step, which):
        for m in range(2):
            zfield[m] = jnp.where(slot >= 2, zrecv[step, which, 1, m], zrecv[step, which, 0, m])

    def phase_a(made, field, zfield, step):
        start(made, X1)
        for m in range(2):
            for x in range(cells_x):
                ysend[step, 0, m, 2 * x:2 * x + 2] = field[m, x + 2, low:low + 2]
                ysend[step, 1, m, 2 * x:2 * x + 2] = field[m, x + 2, high - 2:high]
        start(made, Y)
        pack_z(field, step, 0)
        start(made, Z)
        start(made, X2)
        arrive(made, Y)
        for m in range(2):
            for x in range(cells_x):
                field[m, x + 2, low - 2:low] = yrecv[step, 1, m, 2 * x:2 * x + 2]
                field[m, x + 2, high:high + 2] = yrecv[step, 0, m, 2 * x:2 * x + 2]
        arrive(made, Z)
        unpack_z(zfield, step, 0)
        arrive(made, X1)

    def phase_b_start(made, field, step):
        for m in range(2):
            for side, xi in enumerate((1, cells_x + 2)):
                at = 2 * m + side
                yesend[step, 0, at:at + 1] = field[m, xi, low:low + 1]
                yesend[step, 1, at:at + 1] = field[m, xi, high - 1:high]
        start(made, YE)
        pack_z(field, step, 1)
        start(made, ZE)

    def phase_b_end(made, field, zfield, step):
        arrive(made, YE)
        for m in range(2):
            for side, xi in enumerate((1, cells_x + 2)):
                at = 2 * m + side
                field[m, xi, low - 1:low] = yerecv[step, 1, at:at + 1]
                field[m, xi, high:high + 1] = yerecv[step, 0, at:at + 1]
        arrive(made, ZE)
        unpack_z(zfield, step, 1)
        arrive(made, X2)

    def turn(packed, xi):
        return pltpu.roll(packed, lanes - 2 - 4 * xi, 1)

    def up(v, halo):
        return jnp.where(lane_row == lanes - 1, halo, pltpu.roll(v, lanes - 1, 1))

    def down(v, halo):
        return jnp.where(lane_row == 0, halo, pltpu.roll(v, 1, 1))

    def cross(a, b, k):
        i, j = (k + 1) % 3, (k + 2) % 3
        return a[i] * b[j] - a[j] * b[i]

    def flux_pass():
        def z_halo():
            diffs = []
            rows, above, below = own, pl.ds(low + 1, cells_y), pl.ds(low - 1, cells_y)
            for m in range(2):
                halo, edge = zcur[m, rows], pack[m, rows]
                diffs.append((
                    pltpu.roll(halo, lanes - 4, 1) - pltpu.roll(halo, 4, 1),
                    zcur[m, above] - zcur[m, below],
                    jnp.where(slot == 1, pltpu.roll(halo, 1, 1) - edge, edge - pltpu.roll(halo, lanes - 1, 1))))
            a, b = diffs
            crossed = [cross(a, b, k) for k in range(3)]
            fz[0, :] = cross(b, crossed, 2)
            fz[1, :] = cross(crossed, a, 2)

        z_halo()

        def rows_flux(xi, first, count, comps):
            rows = pl.ds(first, count)
            diffs = []
            for m in range(2):
                v = cur[m, xi, rows]
                halo = turn(zcur[m, rows], xi)
                diffs.append((
                    cur[m, xi + 1, rows] - cur[m, xi - 1, rows],
                    cur[m, xi, pl.ds(first + 1, count)] - cur[m, xi, pl.ds(first - 1, count)],
                    up(v, halo) - down(v, halo)))
            a, b = diffs
            crossed = [cross(a, b, k) for k in range(3)]
            for k in comps:
                one, two = cross(b, crossed, k), cross(crossed, a, k)
                if k == 0:
                    f0[0, xi], f0[1, xi] = one, two
                elif k == 1:
                    f1[0, xi, rows], f1[1, xi, rows] = one, two
                else:
                    f2[0, xi], f2[1, xi] = one, two

        def body(xi, carry):
            rows_flux(xi, low, cells_y, (0, 1, 2))
            rows_flux(xi, low - 1, 1, (1,))
            rows_flux(xi, high, 1, (1,))
            return carry

        rows_flux(1, low, cells_y, (0,))
        lax.fori_loop(2, cells_x + 2, body, 0)
        rows_flux(cells_x + 2, low, cells_y, (0,))

    def fold(v):
        return jnp.sum(v.reshape(cells_y // 8, 8, lanes), axis=0)

    def laplace(field, zfield, m, xi):
        v = field[m, xi, own]
        halo = turn(zfield[m, own], xi)
        around = field[m, xi + 1, own] + field[m, xi - 1, own]
        around = around + (field[m, xi, pl.ds(low + 1, cells_y)] + field[m, xi, pl.ds(low - 1, cells_y)])
        return v, 6.0 * v - (around + (up(v, halo) + down(v, halo)))

    def gradient_pass(step):
        def body(xi, norm):
            for m in range(2):
                v, smooth = laplace(cur, zcur, m, xi)
                inner = f2[m, xi]
                halo = turn(fz[m], xi)
                div = f0[m, xi + 1] - f0[m, xi - 1]
                div = div + (f1[m, xi, pl.ds(low + 1, cells_y)] - f1[m, xi, pl.ds(low - 1, cells_y)])
                div = div + (up(inner, halo) - down(inner, halo))
                g = weights[m, xi - 2] * (v - targets[m, xi - 2]) + smooth + COUPLE * div
                grad[step, m, xi, own] = g
                norm = norm + fold(g * g)
            return norm

        return lax.fori_loop(2, cells_x + 2, body, jnp.zeros((8, lanes), jnp.float32))

    def curvature_pass(step):
        def body(xi, curve):
            for m in range(2):
                v, smooth = laplace(grad.at[step], zgrad, m, xi)
                turned = weights[m, xi - 2] * v + smooth
                if step == ITERS - 1:
                    applied[m, xi - 2] = turned
                curve = curve + fold(v * turned)
            return curve

        return lax.fori_loop(2, cells_x + 2, body, jnp.zeros((8, lanes), jnp.float32))

    def red_copy(step, k):
        peer = lax.rem(me + k, total)
        there = (peer // (ny * nz), lax.rem(peer // nz, ny), lax.rem(peer, nz))
        return pltpu.make_async_remote_copy(
            src_ref=red.at[step, me], dst_ref=red.at[step, me], send_sem=red_send.at[step], recv_sem=red_recv.at[step],
            device_id=there, device_id_type=MESH)

    def reduce_start(step, norm, curve):
        row = jnp.where(lane_row < lanes // 2, jnp.sum(norm), jnp.sum(curve))
        red[step, me] = row

        def body(k, carry):
            red_copy(step, k).start()
            return carry

        lax.fori_loop(1, total, body, 0)

    def reduce_wait(step, sem):
        part = red.at[step, pl.ds(0, total - 1)]
        pltpu.make_async_copy(part, part, sem.at[step]).wait()

    def reduce_end(step):
        reduce_wait(step, red_recv)
        summed = jnp.sum(red[step], axis=0)
        ratio = summed / pltpu.roll(summed, lanes // 2, 1)
        return jnp.where(lane_row < lanes // 2, ratio, pltpu.roll(ratio, lanes // 2, 1))

    first, last = transfers(0, cur), []
    zgrad[...] = jnp.zeros_like(zgrad)
    for m in range(2):
        def load(xi, carry):
            cur[m, xi, own] = models[m, xi - 2]
            return carry
        lax.fori_loop(2, cells_x + 2, load, 0)
    phase_a(first, cur, zcur, 0)
    phase_b_start(first, cur, 0)
    phase_b_end(first, cur, zcur, 0)
    last.append((first, True))

    for step in range(ITERS):
        final = step == ITERS - 1
        flux_pass()
        norm = gradient_pass(step)
        field = grad.at[step]
        made = transfers(step + 1, field)
        phase_a(made, field, zgrad, step + 1)
        curve = curvature_pass(step)
        reduce_start(step, norm, curve)
        last.append((made, not final))
        if not final:
            phase_b_start(made, field, step + 1)
            phase_b_end(made, field, zgrad, step + 1)
            alpha = reduce_end(step)
            if step == 0:
                sent(first, X1)
                sent(first, X2)

            def move(xi, carry):
                for m in range(2):
                    cur[m, xi] = cur[m, xi] - alpha * grad[step, m, xi]
                return carry

            lax.fori_loop(0, cells_x + 4, move, 0)
            for m in range(2):
                zcur[m] = zcur[m] - alpha * zgrad[m]
            pack_z(cur, 0, 2)
        else:
            arrive(made, X2)
            alpha = reduce_end(step)

            def finish(x, carry):
                for m in range(2):
                    updated[m, x] = cur[m, x + 2, own] - alpha * grad[step, m, x + 2, own]
                return carry

            lax.fori_loop(0, cells_x, finish, 0)

    for made, both in last:
        faces = (Y, Z) if made is first else (X1, X2, Y, Z)
        for kind in faces + ((YE, ZE) if both else ()):
            sent(made, kind)
    for step in range(ITERS):
        reduce_wait(step, red_send)


def clearing(sizes, *refs):
    models, targets, weights, updated, applied, cur, grad = refs[:7]
    yrecv, yesend, yerecv, zrecv = refs[14], refs[15], refs[16], refs[18]
    for ref in (yrecv, yesend, yerecv, zrecv):
        ref[...] = jnp.zeros(ref.shape, jnp.float32)
    cells_x = models.shape[1]

    def body(xi, carry):
        for m in range(2):
            cur[m, xi] = jnp.zeros(cur.shape[2:], jnp.float32)
            for step in range(ITERS):
                grad[step, m, xi] = jnp.zeros(cur.shape[2:], jnp.float32)
        return carry

    lax.fori_loop(0, cells_x + 4, body, 0)
    total = sizes[0] * sizes[1] * sizes[2]
    ix, iy, iz = (lax.axis_index(axis) for axis in AXES)
    me = (ix * sizes[1] + iy) * sizes[2] + iz
    barrier = pltpu.get_barrier_semaphore()

    def greet(k, carry):
        peer = lax.rem(me + k, total)
        there = (peer // (sizes[1] * sizes[2]), lax.rem(peer // sizes[2], sizes[1]), lax.rem(peer, sizes[2]))
        pl.semaphore_signal(barrier, inc=1, device_id=there, device_id_type=MESH)
        return carry

    lax.fori_loop(1, total, greet, 0)
    pl.semaphore_wait(barrier, total - 1)
    kernel(sizes, *refs)


def solution(mesh):
    sizes = tuple(mesh.shape[axis] for axis in AXES)

    def local(models, targets, weights):
        _, nx, ny, nz = models.shape
        rows = ny + 16
        total = sizes[0] * sizes[1] * sizes[2]
        steps = ITERS + 1
        whole = pl.BlockSpec(memory_space=pltpu.VMEM)
        f32 = jnp.float32
        return pl.pallas_call(
            functools.partial(clearing, sizes),
            out_shape=(jax.ShapeDtypeStruct(models.shape, f32),) * 2,
            in_specs=[whole] * 3,
            out_specs=(whole, whole),
            scratch_shapes=[
                pltpu.VMEM((2, nx + 4, rows, nz), f32),
                pltpu.VMEM((ITERS, 2, nx + 4, rows, nz), f32),
                pltpu.VMEM((2, rows, nz), f32),
                pltpu.VMEM((2, rows, nz), f32),
                pltpu.VMEM((2, rows, nz), f32),
                pltpu.VMEM((2, nx + 4, ny, nz), f32),
                pltpu.VMEM((2, nx + 4, rows, nz), f32),
                pltpu.VMEM((2, nx + 4, ny, nz), f32),
                pltpu.VMEM((2, ny, nz), f32),
                pltpu.VMEM((steps, 2, 2, 2 * nx, nz), f32),
                pltpu.VMEM((steps, 2, 2, 2 * nx, nz), f32),
                pltpu.VMEM((steps, 2, 8, nz), f32),
                pltpu.VMEM((steps, 2, 8, nz), f32),
                pltpu.VMEM((steps, 3, 2, rows, nz), f32),
                pltpu.VMEM((steps, 2, 2, 2, rows, nz), f32),
                pltpu.VMEM((ITERS, total, 1, nz), f32),
                pltpu.SemaphoreType.DMA((steps, 12)),
                pltpu.SemaphoreType.DMA((steps, 12)),
                pltpu.SemaphoreType.DMA((ITERS,)),
                pltpu.SemaphoreType.DMA((ITERS,)),
            ],
            compiler_params=pltpu.CompilerParams(
                collective_id=0, has_side_effects=True, vmem_limit_bytes=48 * 1024 * 1024),
        )(models, targets, weights)

    spec = P(None, *AXES)
    return jax.shard_map(local, mesh=mesh, in_specs=(spec,) * 3, out_specs=(spec, spec), check_vma=False)
```

```python
import functools

import jax
import jax.numpy as jnp
from jax import lax
from jax.experimental import pallas as pl
from jax.experimental.pallas import tpu as pltpu
from jax.sharding import PartitionSpec as P

ITERS = 3
AXES = ("gx", "gy", "gz")
MESH = pl.DeviceIdType.MESH
X1, X2, Y, Z, YE, ZE = 0, 2, 4, 6, 8, 10
COUPLE = -2.0 * 0.05 / 16.0


def kernel(sizes, models, targets_in, weights_in, updated, applied, cur, grad, zcur, zgrad, pack, f0, f1, f2, fz,
           ysend, yrecv, yesend, yerecv, zsend, zrecv, targets, weights, red, line, send, recv, red_send, red_recv,
           line_send, line_recv, fetched):
    nx, ny, nz = sizes
    _, cells_x, cells_y, lanes = models.shape
    low, high = 8, 8 + cells_y
    own = pl.ds(low, cells_y)
    ix, iy, iz = (lax.axis_index(axis) for axis in AXES)
    here = (ix, iy, iz)
    lane_row = lax.broadcasted_iota(jnp.int32, (1, lanes), 1)
    slot = lax.rem(lane_row, 4)

    def has(axis, direction):
        return here[axis] > 0 if direction == 0 else here[axis] < sizes[axis] - 1

    def copy(step, axis, direction, kind, src, dst):
        there = list(here)
        there[axis] = here[axis] + (1 if direction else -1)
        return pltpu.make_async_remote_copy(
            src_ref=src, dst_ref=dst, send_sem=send.at[step, kind + direction], recv_sem=recv.at[step, kind + direction],
            device_id=tuple(there), device_id_type=MESH)

    def transfers(step, field):
        made = {}
        for direction in range(2):
            near, far = (2, cells_x + 2) if direction == 0 else (cells_x + 1, 1)
            made[X1, direction] = (0, field.at[:, near, own], field.at[:, far, own])
            near, far = (3, cells_x + 3) if direction == 0 else (cells_x, 0)
            made[X2, direction] = (0, field.at[:, near, own], field.at[:, far, own])
            made[Y, direction] = (1, ysend.at[step, direction], yrecv.at[step, direction])
            made[YE, direction] = (1, yesend.at[step, direction], yerecv.at[step, direction])
            made[Z, direction] = (2, zsend.at[step, 0], zrecv.at[step, 0, direction])
            made[ZE, direction] = (2, zsend.at[step, 1], zrecv.at[step, 1, direction])
        return {key: (value[0], copy(step, value[0], key[1], key[0], value[1], value[2])) for key, value in made.items()}

    def start(made, kind):
        for direction in range(2):
            axis, move = made[kind, direction]

            @pl.when(has(axis, direction))
            def _():
                move.start()

    def arrive(made, kind):
        for direction in range(2):
            axis, move = made[kind, direction]

            @pl.when(has(axis, 1 - direction))
            def _():
                move.wait_recv()

    def sent(made, kind):
        for direction in range(2):
            axis, move = made[kind, direction]

            @pl.when(has(axis, direction))
            def _():
                move.wait_send()

    def pack_z(field, step, which):
        group = lane_row // 4

        def body(xi, carry):
            return tuple(
                jnp.where(group == xi, pltpu.roll(field[m, xi], 4 * xi + 2, 1), carry[m]) for m in range(2))

        zero = jnp.zeros(field.shape[2:], jnp.float32)
        edge = 2 if which == 0 else 1
        packed = lax.fori_loop(edge, cells_x + 4 - edge, body, (zero, zero))
        for m in range(2):
            v = packed[m]
            pack[m] = v
            turned = jnp.where(slot == 0, pltpu.roll(v, lanes - 3, 1), pltpu.roll(v, 3, 1))
            turned = jnp.where(slot == 1, pltpu.roll(v, lanes - 1, 1), turned)
            zsend[step, which, m] = jnp.where(slot == 2, pltpu.roll(v, 1, 1), turned)

    def unpack_z(zfield, step, which):
        for m in range(2):
            zfield[m] = jnp.where(slot >= 2, zrecv[step, which, 1, m], zrecv[step, which, 0, m])

    def phase_a(made, field, zfield, step):
        start(made, X1)
        for m in range(2):
            for x in range(cells_x):
                ysend[step, 0, m, 2 * x:2 * x + 2] = field[m, x + 2, low:low + 2]
                ysend[step, 1, m, 2 * x:2 * x + 2] = field[m, x + 2, high - 2:high]
        start(made, Y)
        pack_z(field, step, 0)
        start(made, Z)
        start(made, X2)
        arrive(made, Y)
        arrive(made, Z)
        unpack_z(zfield, step, 0)
        arrive(made, X1)

    def unpack_y(field, step):
        for m in range(2):
            for x in range(cells_x):
                field[m, x + 2, low - 2:low] = yrecv[step, 1, m, 2 * x:2 * x + 2]
                field[m, x + 2, high:high + 2] = yrecv[step, 0, m, 2 * x:2 * x + 2]

    def face_terms(field, step):
        row = lax.broadcasted_iota(jnp.int32, (2 * cells_x, 1), 0)
        even = lax.rem(row, 2) == 0
        inner = jnp.logical_or(slot == 1, slot == 2)
        count = 2 * cells_x
        terms = jnp.zeros((8, lanes), jnp.float32)
        for m in range(2):
            terms = terms + fold(field[m, 2, own] * field[m, 1, own] + field[m, cells_x + 1, own] * field[m, cells_x + 2, own])
            before = ysend[step, 0, m] * pltpu.roll(yrecv[step, 1, m], count - 1, 0)
            after = ysend[step, 1, m] * pltpu.roll(yrecv[step, 0, m], 1, 0)
            terms = terms + jnp.sum(jnp.where(even, before, after).reshape(count // 8, 8, lanes), axis=0)
            terms = terms + fold(jnp.where(inner, pack[m, own] * zgrad[m, own], 0.0))
        return terms

    def phase_b_start(made, field, step):
        for m in range(2):
            for side, xi in enumerate((1, cells_x + 2)):
                at = 2 * m + side
                yesend[step, 0, at:at + 1] = field[m, xi, low:low + 1]
                yesend[step, 1, at:at + 1] = field[m, xi, high - 1:high]
        start(made, YE)

    def phase_b_end(made, field, zfield, step):
        arrive(made, YE)
        for m in range(2):
            for side, xi in enumerate((1, cells_x + 2)):
                at = 2 * m + side
                field[m, xi, low - 1:low] = yerecv[step, 1, at:at + 1]
                field[m, xi, high:high + 1] = yerecv[step, 0, at:at + 1]
        arrive(made, ZE)
        unpack_z(zfield, step, 1)
        arrive(made, X2)

    def turn(packed, xi):
        return pltpu.roll(packed, lanes - 2 - 4 * xi, 1)

    def up(v, halo):
        return jnp.where(lane_row == lanes - 1, halo, pltpu.roll(v, lanes - 1, 1))

    def down(v, halo):
        return jnp.where(lane_row == 0, halo, pltpu.roll(v, 1, 1))

    def cross(a, b, k):
        i, j = (k + 1) % 3, (k + 2) % 3
        return a[i] * b[j] - a[j] * b[i]

    def flux_pass():
        def z_halo():
            diffs = []
            rows, above, below = own, pl.ds(low + 1, cells_y), pl.ds(low - 1, cells_y)
            for m in range(2):
                halo, edge = zcur[m, rows], pack[m, rows]
                diffs.append((
                    pltpu.roll(halo, lanes - 4, 1) - pltpu.roll(halo, 4, 1),
                    zcur[m, above] - zcur[m, below],
                    jnp.where(slot == 1, pltpu.roll(halo, 1, 1) - edge, edge - pltpu.roll(halo, lanes - 1, 1))))
            a, b = diffs
            crossed = [cross(a, b, k) for k in range(3)]
            fz[0, :] = cross(b, crossed, 2)
            fz[1, :] = cross(crossed, a, 2)

        z_halo()

        def rows_flux(xi, first, count, comps):
            rows = pl.ds(first, count)
            diffs = []
            for m in range(2):
                v = cur[m, xi, rows]
                halo = turn(zcur[m, rows], xi)
                diffs.append((
                    cur[m, xi + 1, rows] - cur[m, xi - 1, rows],
                    cur[m, xi, pl.ds(first + 1, count)] - cur[m, xi, pl.ds(first - 1, count)],
                    up(v, halo) - down(v, halo)))
            a, b = diffs
            crossed = [cross(a, b, k) for k in range(3)]
            for k in comps:
                one, two = cross(b, crossed, k), cross(crossed, a, k)
                if k == 0:
                    f0[0, xi], f0[1, xi] = one, two
                elif k == 1:
                    f1[0, xi, rows], f1[1, xi, rows] = one, two
                else:
                    f2[0, xi], f2[1, xi] = one, two

        def body(xi, carry):
            rows_flux(xi, low, cells_y, (0, 1, 2))
            rows_flux(xi, low - 1, 1, (1,))
            rows_flux(xi, high, 1, (1,))
            return carry

        rows_flux(1, low, cells_y, (0,))
        lax.fori_loop(2, cells_x + 2, body, 0)
        rows_flux(cells_x + 2, low, cells_y, (0,))

    def fold(v):
        return jnp.sum(v.reshape(cells_y // 8, 8, lanes), axis=0)

    def laplace(field, zfield, m, xi):
        v = field[m, xi, own]
        halo = turn(zfield[m, own], xi)
        around = field[m, xi + 1, own] + field[m, xi - 1, own]
        around = around + (field[m, xi, pl.ds(low + 1, cells_y)] + field[m, xi, pl.ds(low - 1, cells_y)])
        return v, 6.0 * v - (around + (up(v, halo) + down(v, halo)))

    def gradient_pass(step):
        def body(xi, carry):
            norm, curve, edges, before = carry
            kept = []
            for m in range(2):
                v, smooth = laplace(cur, zcur, m, xi)
                inner = f2[m, xi]
                halo = turn(fz[m], xi)
                div = f0[m, xi + 1] - f0[m, xi - 1]
                div = div + (f1[m, xi, pl.ds(low + 1, cells_y)] - f1[m, xi, pl.ds(low - 1, cells_y)])
                div = div + (up(inner, halo) - down(inner, halo))
                weight = weights[m, xi - 2]
                g = weight * (v - targets[m, xi - 2]) + smooth + COUPLE * div
                grad[step, m, xi, own] = g
                square = g * g
                norm = norm + fold(square)
                curve = curve + fold((weight + 6.0) * square)
                later = jnp.where(row_in == cells_y - 1, 0.0, pltpu.roll(g, cells_y - 1, 0))
                beside = jnp.where(lane_row == lanes - 1, 0.0, pltpu.roll(g, lanes - 1, 1))
                edges = edges + fold(g * (before[m] + later + beside))
                kept.append(g)
            return norm, curve, edges, tuple(kept)

        row_in = lax.broadcasted_iota(jnp.int32, (cells_y, 1), 0)
        zero, slab = jnp.zeros((8, lanes), jnp.float32), jnp.zeros((cells_y, lanes), jnp.float32)
        norm, curve, edges, _ = lax.fori_loop(2, cells_x + 2, body, (zero, zero, zero, (slab, slab)))
        return norm, curve - 2.0 * edges

    def applied_pass(step):
        def body(xi, carry):
            for m in range(2):
                v, smooth = laplace(grad.at[step], zgrad, m, xi)
                applied[m, xi - 2] = weights[m, xi - 2] * v + smooth
            return carry

        lax.fori_loop(2, cells_x + 2, body, 0)

    plane, place = ny * nz, iy * nz + iz

    def plane_copy(step, k):
        peer = lax.rem(place + k, plane)
        return pltpu.make_async_remote_copy(
            src_ref=red.at[step, place], dst_ref=red.at[step, place], send_sem=red_send.at[step],
            recv_sem=red_recv.at[step], device_id=(ix, peer // nz, lax.rem(peer, nz)), device_id_type=MESH)

    def line_copy(step, k):
        return pltpu.make_async_remote_copy(
            src_ref=line.at[step, ix], dst_ref=line.at[step, ix], send_sem=line_send.at[step],
            recv_sem=line_recv.at[step], device_id=(lax.rem(ix + k, nx), iy, iz), device_id_type=MESH)

    def reduce_wait(ref, step, count, sem):
        if count > 1:
            part = ref.at[step, pl.ds(0, count - 1)]
            pltpu.make_async_copy(part, part, sem.at[step]).wait()

    def reduce_plane(step, norm, curve):
        red[step, place] = jnp.where(lane_row < lanes // 2, jnp.sum(norm), jnp.sum(curve))
        for k in range(1, plane):
            plane_copy(step, k).start()

    def reduce_line(step):
        reduce_wait(red, step, plane, red_recv)
        line[step, ix] = jnp.sum(red[step], axis=0)
        for k in range(1, nx):
            line_copy(step, k).start()

    def reduce_end(step):
        reduce_wait(line, step, nx, line_recv)
        summed = jnp.sum(line[step], axis=0)
        ratio = summed / pltpu.roll(summed, lanes // 2, 1)
        return jnp.where(lane_row < lanes // 2, ratio, pltpu.roll(ratio, lanes // 2, 1))

    fetches = [
        pltpu.make_async_copy(models, cur.at[:, pl.ds(2, cells_x), own], fetched.at[0]),
        pltpu.make_async_copy(weights_in, weights, fetched.at[1]),
        pltpu.make_async_copy(targets_in, targets, fetched.at[2]),
    ]
    for fetch in fetches:
        fetch.start()
    for ref in (yrecv, yesend, yerecv, zrecv):
        ref[...] = jnp.zeros(ref.shape, jnp.float32)
    blank = jnp.zeros(cur.shape[2:], jnp.float32)
    for m in range(2):
        for xi in (0, 1, cells_x + 2, cells_x + 3):
            cur[m, xi] = blank
            for step in range(ITERS):
                grad[step, m, xi] = blank
    barrier = pltpu.get_barrier_semaphore()
    for k in range(1, plane):
        peer = lax.rem(place + k, plane)
        pl.semaphore_signal(
            barrier, inc=1, device_id=(ix, peer // nz, lax.rem(peer, nz)), device_id_type=MESH)
    for k in range(1, nx):
        pl.semaphore_signal(barrier, inc=1, device_id=(lax.rem(ix + k, nx), iy, iz), device_id_type=MESH)
    strip = jnp.zeros((8, lanes), jnp.float32)

    def clear(xi, carry):
        for m in range(2):
            for at in (0, high):
                cur[m, xi, at:at + 8] = strip
                for step in range(ITERS):
                    grad[step, m, xi, at:at + 8] = strip
        return carry

    lax.fori_loop(2, cells_x + 2, clear, 0)
    zgrad[...] = jnp.zeros_like(zgrad)
    fetches[0].wait()
    pl.semaphore_wait(barrier, plane + nx - 2)

    first, last = transfers(0, cur), []
    phase_a(first, cur, zcur, 0)
    phase_b_start(first, cur, 0)
    unpack_y(cur, 0)
    pack_z(cur, 0, 1)
    start(first, ZE)
    phase_b_end(first, cur, zcur, 0)
    last.append((first, True))
    fetches[1].wait()
    fetches[2].wait()

    for step in range(ITERS):
        final = step == ITERS - 1
        flux_pass()
        norm, curve = gradient_pass(step)
        field = grad.at[step]
        made = transfers(step + 1, field)
        phase_a(made, field, zgrad, step + 1)
        reduce_plane(step, norm, curve - face_terms(field, step + 1))
        last.append((made, not final))
        if not final:
            phase_b_start(made, field, step + 1)
            unpack_y(field, step + 1)
            reduce_line(step)
            pack_z(field, step + 1, 1)
            start(made, ZE)
            phase_b_end(made, field, zgrad, step + 1)
            alpha = reduce_end(step)
            if step == 0:
                sent(first, X1)
                sent(first, X2)

            def move(xi, carry):
                for m in range(2):
                    cur[m, xi] = cur[m, xi] - alpha * grad[step, m, xi]
                return carry

            lax.fori_loop(0, cells_x + 4, move, 0)
            for m in range(2):
                zcur[m] = zcur[m] - alpha * zgrad[m]
            pack_z(cur, 0, 2)
        else:
            unpack_y(field, step + 1)
            reduce_line(step)
            applied_pass(step)
            arrive(made, X2)
            alpha = reduce_end(step)

            def finish(x, carry):
                for m in range(2):
                    updated[m, x] = cur[m, x + 2, own] - alpha * grad[step, m, x + 2, own]
                return carry

            lax.fori_loop(0, cells_x, finish, 0)

    for made, both in last:
        faces = (Y, Z) if made is first else (X1, X2, Y, Z)
        for kind in faces + ((YE, ZE) if both else ()):
            sent(made, kind)
    for step in range(ITERS):
        reduce_wait(red, step, plane, red_send)
        reduce_wait(line, step, nx, line_send)


def solution(mesh):
    sizes = tuple(mesh.shape[axis] for axis in AXES)

    def local(models, targets, weights):
        _, nx, ny, nz = models.shape
        rows = ny + 16
        steps = ITERS + 1
        whole = pl.BlockSpec(memory_space=pltpu.VMEM)
        f32 = jnp.float32
        return pl.pallas_call(
            functools.partial(kernel, sizes),
            out_shape=(jax.ShapeDtypeStruct(models.shape, f32),) * 2,
            in_specs=[pl.BlockSpec(memory_space=pl.ANY)] * 3,
            out_specs=(whole, whole),
            scratch_shapes=[
                pltpu.VMEM((2, nx + 4, rows, nz), f32),
                pltpu.VMEM((ITERS, 2, nx + 4, rows, nz), f32),
                pltpu.VMEM((2, rows, nz), f32),
                pltpu.VMEM((2, rows, nz), f32),
                pltpu.VMEM((2, rows, nz), f32),
                pltpu.VMEM((2, nx + 4, ny, nz), f32),
                pltpu.VMEM((2, nx + 4, rows, nz), f32),
                pltpu.VMEM((2, nx + 4, ny, nz), f32),
                pltpu.VMEM((2, ny, nz), f32),
                pltpu.VMEM((steps, 2, 2, 2 * nx, nz), f32),
                pltpu.VMEM((steps, 2, 2, 2 * nx, nz), f32),
                pltpu.VMEM((steps, 2, 8, nz), f32),
                pltpu.VMEM((steps, 2, 8, nz), f32),
                pltpu.VMEM((steps, 3, 2, rows, nz), f32),
                pltpu.VMEM((steps, 2, 2, 2, rows, nz), f32),
                pltpu.VMEM((2, nx, ny, nz), f32),
                pltpu.VMEM((2, nx, ny, nz), f32),
                pltpu.VMEM((ITERS, sizes[1] * sizes[2], 1, nz), f32),
                pltpu.VMEM((ITERS, sizes[0], 1, nz), f32),
                pltpu.SemaphoreType.DMA((steps, 12)),
                pltpu.SemaphoreType.DMA((steps, 12)),
                pltpu.SemaphoreType.DMA((ITERS,)),
                pltpu.SemaphoreType.DMA((ITERS,)),
                pltpu.SemaphoreType.DMA((ITERS,)),
                pltpu.SemaphoreType.DMA((ITERS,)),
                pltpu.SemaphoreType.DMA((3,)),
            ],
            compiler_params=pltpu.CompilerParams(
                collective_id=0, has_side_effects=True, vmem_limit_bytes=48 * 1024 * 1024),
        )(models, targets, weights)

    spec = P(None, *AXES)
    return jax.shard_map(local, mesh=mesh, in_specs=(spec,) * 3, out_specs=(spec, spec), check_vma=False)
```

```python
import functools

import jax
import jax.numpy as jnp
from jax import lax
from jax.experimental import pallas as pl
from jax.experimental.pallas import tpu as pltpu
from jax.sharding import PartitionSpec as P

ITERS = 3
AXES = ("gx", "gy", "gz")
MESH = pl.DeviceIdType.MESH
X1, X2, Y, Z, YE, ZE = 0, 2, 4, 6, 8, 10
COUPLE = -2.0 * 0.05 / 16.0


def kernel(sizes, models, targets_in, weights_in, updated, applied, cur, grad, zcur, zgrad, pack, f0, f1, f2, fz,
           ysend, yrecv, yesend, yerecv, zsend, zrecv, targets, weights, red, send, recv, red_send, red_recv,
           fetched):
    nx, ny, nz = sizes
    _, cells_x, cells_y, lanes = models.shape
    low, high = 8, 8 + cells_y
    own = pl.ds(low, cells_y)
    ix, iy, iz = (lax.axis_index(axis) for axis in AXES)
    here = (ix, iy, iz)
    lane_row = lax.broadcasted_iota(jnp.int32, (1, lanes), 1)
    slot = lax.rem(lane_row, 4)

    def has(axis, direction):
        return here[axis] > 0 if direction == 0 else here[axis] < sizes[axis] - 1

    def copy(step, axis, direction, kind, src, dst):
        there = list(here)
        there[axis] = here[axis] + (1 if direction else -1)
        return pltpu.make_async_remote_copy(
            src_ref=src, dst_ref=dst, send_sem=send.at[step, kind + direction], recv_sem=recv.at[step, kind + direction],
            device_id=tuple(there), device_id_type=MESH)

    def transfers(step, field):
        made = {}
        for direction in range(2):
            near, far = (2, cells_x + 2) if direction == 0 else (cells_x + 1, 1)
            made[X1, direction] = (0, field.at[:, near, own], field.at[:, far, own])
            near, far = (3, cells_x + 3) if direction == 0 else (cells_x, 0)
            made[X2, direction] = (0, field.at[:, near, own], field.at[:, far, own])
            made[Y, direction] = (1, ysend.at[step, direction], yrecv.at[step, direction])
            made[YE, direction] = (1, yesend.at[step, direction], yerecv.at[step, direction])
            made[Z, direction] = (2, zsend.at[step, 0], zrecv.at[step, 0, direction])
            made[ZE, direction] = (2, zsend.at[step, 1], zrecv.at[step, 1, direction])
        return {key: (value[0], copy(step, value[0], key[1], key[0], value[1], value[2])) for key, value in made.items()}

    def start(made, kind):
        for direction in range(2):
            axis, move = made[kind, direction]

            @pl.when(has(axis, direction))
            def _():
                move.start()

    def arrive(made, kind):
        for direction in range(2):
            axis, move = made[kind, direction]

            @pl.when(has(axis, 1 - direction))
            def _():
                move.wait_recv()

    def sent(made, kind):
        for direction in range(2):
            axis, move = made[kind, direction]

            @pl.when(has(axis, direction))
            def _():
                move.wait_send()

    def pack_z(field, step, which):
        group = lane_row // 4

        def body(xi, carry):
            return tuple(
                jnp.where(group == xi, pltpu.roll(field[m, xi], 4 * xi + 2, 1), carry[m]) for m in range(2))

        zero = jnp.zeros(field.shape[2:], jnp.float32)
        edge = 2 if which == 0 else 1
        packed = (zero, zero)
        for xi in range(edge, cells_x + 4 - edge):
            packed = body(xi, packed)
        for m in range(2):
            v = packed[m]
            pack[m] = v
            turned = jnp.where(slot == 0, pltpu.roll(v, lanes - 3, 1), pltpu.roll(v, 3, 1))
            turned = jnp.where(slot == 1, pltpu.roll(v, lanes - 1, 1), turned)
            zsend[step, which, m] = jnp.where(slot == 2, pltpu.roll(v, 1, 1), turned)

    def unpack_z(zfield, step, which):
        for m in range(2):
            zfield[m] = jnp.where(slot >= 2, zrecv[step, which, 1, m], zrecv[step, which, 0, m])

    def phase_a(made, field, zfield, step):
        start(made, X1)
        for m in range(2):
            for x in range(cells_x):
                ysend[step, 0, m, 2 * x:2 * x + 2] = field[m, x + 2, low:low + 2]
                ysend[step, 1, m, 2 * x:2 * x + 2] = field[m, x + 2, high - 2:high]
        start(made, Y)
        pack_z(field, step, 0)
        start(made, Z)
        start(made, X2)
        arrive(made, Y)
        arrive(made, Z)
        unpack_z(zfield, step, 0)
        arrive(made, X1)

    def unpack_y(field, step):
        for m in range(2):
            for x in range(cells_x):
                field[m, x + 2, low - 2:low] = yrecv[step, 1, m, 2 * x:2 * x + 2]
                field[m, x + 2, high:high + 2] = yrecv[step, 0, m, 2 * x:2 * x + 2]

    def face_terms(field, step):
        row = lax.broadcasted_iota(jnp.int32, (2 * cells_x, 1), 0)
        even = lax.rem(row, 2) == 0
        inner = jnp.logical_or(slot == 1, slot == 2)
        count = 2 * cells_x
        terms = jnp.zeros((8, lanes), jnp.float32)
        for m in range(2):
            terms = terms + fold(field[m, 2, own] * field[m, 1, own] + field[m, cells_x + 1, own] * field[m, cells_x + 2, own])
            before = ysend[step, 0, m] * pltpu.roll(yrecv[step, 1, m], count - 1, 0)
            after = ysend[step, 1, m] * pltpu.roll(yrecv[step, 0, m], 1, 0)
            terms = terms + jnp.sum(jnp.where(even, before, after).reshape(count // 8, 8, lanes), axis=0)
            terms = terms + fold(jnp.where(inner, pack[m, own] * zgrad[m, own], 0.0))
        return terms

    def phase_b_start(made, field, step):
        for m in range(2):
            for side, xi in enumerate((1, cells_x + 2)):
                at = 2 * m + side
                yesend[step, 0, at:at + 1] = field[m, xi, low:low + 1]
                yesend[step, 1, at:at + 1] = field[m, xi, high - 1:high]
        start(made, YE)

    def phase_b_end(made, field, zfield, step):
        arrive(made, YE)
        for m in range(2):
            for side, xi in enumerate((1, cells_x + 2)):
                at = 2 * m + side
                field[m, xi, low - 1:low] = yerecv[step, 1, at:at + 1]
                field[m, xi, high:high + 1] = yerecv[step, 0, at:at + 1]
        arrive(made, ZE)
        unpack_z(zfield, step, 1)
        arrive(made, X2)

    def turn(packed, xi):
        return pltpu.roll(packed, lanes - 2 - 4 * xi, 1)

    def up(v, halo):
        return jnp.where(lane_row == lanes - 1, halo, pltpu.roll(v, lanes - 1, 1))

    def down(v, halo):
        return jnp.where(lane_row == 0, halo, pltpu.roll(v, 1, 1))

    def cross(a, b, k):
        i, j = (k + 1) % 3, (k + 2) % 3
        return a[i] * b[j] - a[j] * b[i]

    def flux_pass():
        def z_halo():
            diffs = []
            rows, above, below = own, pl.ds(low + 1, cells_y), pl.ds(low - 1, cells_y)
            for m in range(2):
                halo, edge = zcur[m, rows], pack[m, rows]
                diffs.append((
                    pltpu.roll(halo, lanes - 4, 1) - pltpu.roll(halo, 4, 1),
                    zcur[m, above] - zcur[m, below],
                    jnp.where(slot == 1, pltpu.roll(halo, 1, 1) - edge, edge - pltpu.roll(halo, lanes - 1, 1))))
            a, b = diffs
            crossed = [cross(a, b, k) for k in range(3)]
            fz[0, :] = cross(b, crossed, 2)
            fz[1, :] = cross(crossed, a, 2)

        z_halo()

        def rows_flux(xi, first, count, comps):
            rows = pl.ds(first, count)
            diffs = []
            for m in range(2):
                v = cur[m, xi, rows]
                halo = turn(zcur[m, rows], xi)
                diffs.append((
                    cur[m, xi + 1, rows] - cur[m, xi - 1, rows],
                    cur[m, xi, pl.ds(first + 1, count)] - cur[m, xi, pl.ds(first - 1, count)],
                    up(v, halo) - down(v, halo)))
            a, b = diffs
            crossed = [cross(a, b, k) for k in range(3)]
            for k in comps:
                one, two = cross(b, crossed, k), cross(crossed, a, k)
                if k == 0:
                    f0[0, xi], f0[1, xi] = one, two
                elif k == 1:
                    f1[0, xi, rows], f1[1, xi, rows] = one, two
                else:
                    f2[0, xi], f2[1, xi] = one, two

        def body(xi, carry):
            rows_flux(xi, low, cells_y, (0, 1, 2))
            rows_flux(xi, low - 1, 1, (1,))
            rows_flux(xi, high, 1, (1,))
            return carry

        rows_flux(1, low, cells_y, (0,))
        lax.fori_loop(2, cells_x + 2, body, 0, unroll=4)
        rows_flux(cells_x + 2, low, cells_y, (0,))

    def fold(v):
        return jnp.sum(v.reshape(cells_y // 8, 8, lanes), axis=0)

    def laplace(field, zfield, m, xi):
        v = field[m, xi, own]
        halo = turn(zfield[m, own], xi)
        around = field[m, xi + 1, own] + field[m, xi - 1, own]
        around = around + (field[m, xi, pl.ds(low + 1, cells_y)] + field[m, xi, pl.ds(low - 1, cells_y)])
        return v, 6.0 * v - (around + (up(v, halo) + down(v, halo)))

    def gradient_pass(step):
        def body(xi, carry):
            norm, curve, edges, before = carry
            kept = []
            for m in range(2):
                v, smooth = laplace(cur, zcur, m, xi)
                inner = f2[m, xi]
                halo = turn(fz[m], xi)
                div = f0[m, xi + 1] - f0[m, xi - 1]
                div = div + (f1[m, xi, pl.ds(low + 1, cells_y)] - f1[m, xi, pl.ds(low - 1, cells_y)])
                div = div + (up(inner, halo) - down(inner, halo))
                weight = weights[m, xi - 2]
                g = weight * (v - targets[m, xi - 2]) + smooth + COUPLE * div
                grad[step, m, xi, own] = g
                square = g * g
                norm = norm + fold(square)
                curve = curve + fold((weight + 6.0) * square)
                later = jnp.where(row_in == cells_y - 1, 0.0, pltpu.roll(g, cells_y - 1, 0))
                beside = jnp.where(lane_row == lanes - 1, 0.0, pltpu.roll(g, lanes - 1, 1))
                edges = edges + fold(g * (before[m] + later + beside))
                kept.append(g)
            return norm, curve, edges, tuple(kept)

        row_in = lax.broadcasted_iota(jnp.int32, (cells_y, 1), 0)
        zero, slab = jnp.zeros((8, lanes), jnp.float32), jnp.zeros((cells_y, lanes), jnp.float32)
        norm, curve, edges, _ = lax.fori_loop(2, cells_x + 2, body, (zero, zero, zero, (slab, slab)), unroll=4)
        return norm, curve - 2.0 * edges

    def applied_pass(step):
        def body(xi, carry):
            for m in range(2):
                v, smooth = laplace(grad.at[step], zgrad, m, xi)
                applied[m, xi - 2] = weights[m, xi - 2] * v + smooth
            return carry

        lax.fori_loop(2, cells_x + 2, body, 0, unroll=4)

    plane, place = nx * ny * nz, (ix * ny + iy) * nz + iz

    def plane_copy(step, k):
        peer = lax.rem(place + k, plane)
        return pltpu.make_async_remote_copy(
            src_ref=red.at[step, place], dst_ref=red.at[step, place], send_sem=red_send.at[step],
            recv_sem=red_recv.at[step], device_id=(peer // (ny * nz), lax.rem(peer // nz, ny), lax.rem(peer, nz)), device_id_type=MESH)

    def reduce_wait(ref, step, count, sem):
        if count > 1:
            part = ref.at[step, pl.ds(0, count - 1)]
            pltpu.make_async_copy(part, part, sem.at[step]).wait()

    def reduce_plane(step, norm, curve):
        red[step, place] = jnp.where(lane_row < lanes // 2, jnp.sum(norm), jnp.sum(curve))
        for k in range(1, plane):
            plane_copy(step, k).start()

    def reduce_end(step):
        reduce_wait(red, step, plane, red_recv)
        summed = jnp.sum(red[step], axis=0)
        ratio = summed / pltpu.roll(summed, lanes // 2, 1)
        return jnp.where(lane_row < lanes // 2, ratio, pltpu.roll(ratio, lanes // 2, 1))

    fetches = [
        pltpu.make_async_copy(models, cur.at[:, pl.ds(2, cells_x), own], fetched.at[0]),
        pltpu.make_async_copy(weights_in, weights, fetched.at[1]),
        pltpu.make_async_copy(targets_in, targets, fetched.at[2]),
    ]
    for fetch in fetches:
        fetch.start()
    for ref in (yrecv, yesend, yerecv, zrecv):
        ref[...] = jnp.zeros(ref.shape, jnp.float32)
    blank = jnp.zeros(cur.shape[2:], jnp.float32)
    for m in range(2):
        for xi in (0, 1, cells_x + 2, cells_x + 3):
            cur[m, xi] = blank
            for step in range(ITERS):
                grad[step, m, xi] = blank
    barrier = pltpu.get_barrier_semaphore()
    for k in range(1, plane):
        peer = lax.rem(place + k, plane)
        pl.semaphore_signal(
            barrier, inc=1, device_id=(peer // (ny * nz), lax.rem(peer // nz, ny), lax.rem(peer, nz)), device_id_type=MESH)
    strip = jnp.zeros((8, lanes), jnp.float32)

    def clear(xi, carry):
        for m in range(2):
            for at in (0, high):
                cur[m, xi, at:at + 8] = strip
                for step in range(ITERS):
                    grad[step, m, xi, at:at + 8] = strip
        return carry

    lax.fori_loop(2, cells_x + 2, clear, 0)
    zgrad[...] = jnp.zeros_like(zgrad)
    fetches[0].wait()
    pl.semaphore_wait(barrier, plane - 1)

    first, last = transfers(0, cur), []
    phase_a(first, cur, zcur, 0)
    phase_b_start(first, cur, 0)
    unpack_y(cur, 0)
    pack_z(cur, 0, 1)
    start(first, ZE)
    phase_b_end(first, cur, zcur, 0)
    last.append((first, True))
    fetches[1].wait()
    fetches[2].wait()

    for step in range(ITERS):
        final = step == ITERS - 1
        flux_pass()
        norm, curve = gradient_pass(step)
        field = grad.at[step]
        made = transfers(step + 1, field)
        phase_a(made, field, zgrad, step + 1)
        reduce_plane(step, norm, curve - face_terms(field, step + 1))
        last.append((made, not final))
        if not final:
            phase_b_start(made, field, step + 1)
            unpack_y(field, step + 1)
            pack_z(field, step + 1, 1)
            start(made, ZE)
            phase_b_end(made, field, zgrad, step + 1)
            alpha = reduce_end(step)
            if step == 0:
                sent(first, X1)
                sent(first, X2)

            def move(xi, carry):
                for m in range(2):
                    cur[m, xi] = cur[m, xi] - alpha * grad[step, m, xi]
                return carry

            lax.fori_loop(0, cells_x + 4, move, 0, unroll=2)
            for m in range(2):
                zcur[m] = zcur[m] - alpha * zgrad[m]
            pack_z(cur, 0, 2)
        else:
            unpack_y(field, step + 1)
            applied_pass(step)
            arrive(made, X2)
            alpha = reduce_end(step)

            def finish(x, carry):
                for m in range(2):
                    updated[m, x] = cur[m, x + 2, own] - alpha * grad[step, m, x + 2, own]
                return carry

            lax.fori_loop(0, cells_x, finish, 0, unroll=2)

    for made, both in last:
        faces = (Y, Z) if made is first else (X1, X2, Y, Z)
        for kind in faces + ((YE, ZE) if both else ()):
            sent(made, kind)
    for step in range(ITERS):
        reduce_wait(red, step, plane, red_send)


def solution(mesh):
    sizes = tuple(mesh.shape[axis] for axis in AXES)

    def local(models, targets, weights):
        _, nx, ny, nz = models.shape
        rows = ny + 16
        steps = ITERS + 1
        whole = pl.BlockSpec(memory_space=pltpu.VMEM)
        f32 = jnp.float32
        return pl.pallas_call(
            functools.partial(kernel, sizes),
            out_shape=(jax.ShapeDtypeStruct(models.shape, f32),) * 2,
            in_specs=[pl.BlockSpec(memory_space=pl.ANY)] * 3,
            out_specs=(whole, whole),
            scratch_shapes=[
                pltpu.VMEM((2, nx + 4, rows, nz), f32),
                pltpu.VMEM((ITERS, 2, nx + 4, rows, nz), f32),
                pltpu.VMEM((2, rows, nz), f32),
                pltpu.VMEM((2, rows, nz), f32),
                pltpu.VMEM((2, rows, nz), f32),
                pltpu.VMEM((2, nx + 4, ny, nz), f32),
                pltpu.VMEM((2, nx + 4, rows, nz), f32),
                pltpu.VMEM((2, nx + 4, ny, nz), f32),
                pltpu.VMEM((2, ny, nz), f32),
                pltpu.VMEM((steps, 2, 2, 2 * nx, nz), f32),
                pltpu.VMEM((steps, 2, 2, 2 * nx, nz), f32),
                pltpu.VMEM((steps, 2, 8, nz), f32),
                pltpu.VMEM((steps, 2, 8, nz), f32),
                pltpu.VMEM((steps, 3, 2, rows, nz), f32),
                pltpu.VMEM((steps, 2, 2, 2, rows, nz), f32),
                pltpu.VMEM((2, nx, ny, nz), f32),
                pltpu.VMEM((2, nx, ny, nz), f32),
                pltpu.VMEM((ITERS, sizes[0] * sizes[1] * sizes[2], 1, nz), f32),
                pltpu.SemaphoreType.DMA((steps, 12)),
                pltpu.SemaphoreType.DMA((steps, 12)),
                pltpu.SemaphoreType.DMA((ITERS,)),
                pltpu.SemaphoreType.DMA((ITERS,)),
                pltpu.SemaphoreType.DMA((3,)),
            ],
            compiler_params=pltpu.CompilerParams(
                collective_id=0, has_side_effects=True, vmem_limit_bytes=48 * 1024 * 1024),
        )(models, targets, weights)

    spec = P(None, *AXES)
    return jax.shard_map(local, mesh=mesh, in_specs=(spec,) * 3, out_specs=(spec, spec), check_vma=False)
```
